32 devices in a mesh: owner: 4 (over x, core), rows: 8 (over z, y).
Axes of the slice: x: 2, y: 2, z: 4, core: 2. Of those that a mesh axis runs over, the one named last changes fastest.
Arguments:
- master_gate: float32 [64, 2048, 1024], P('owner', 'rows'), may hold values from -0.1875 to 0.1875
- second_gate: bfloat16 [64, 2048, 1024], P('owner', 'rows'), may hold values from -0.0625 to 0.0625
- master_up: float32 [64, 2048, 1024], P('owner', 'rows'), may hold values from -0.1875 to 0.1875
- second_up: bfloat16 [64, 2048, 1024], P('owner', 'rows'), may hold values from -0.0625 to 0.0625
- master_down: float32 [64, 1024, 2048], P('owner', None, 'rows'), may hold values from -0.25 to 0.25
- second_down: bfloat16 [64, 1024, 2048], P('owner', None, 'rows'), may hold values from -0.09375 to 0.09375
- router_weight: float32 [2048, 64], P('rows', 'owner'), may hold values from -0.125 to 0.125
- router_gain: float32 [2048], P('rows'), may hold values from 0.25 to 1.75
Outputs:
- final_gate: bfloat16 [64, 2048, 1024], P('owner', None, 'rows')
- final_up: bfloat16 [64, 2048, 1024], P('owner', None, 'rows')
- final_down: bfloat16 [64, 1024, 2048], P('owner', 'rows')
- scale_gate: float32 [64, 1024], P('owner', 'rows')
- scale_up: float32 [64, 1024], P('owner', 'rows')
- scale_down: float32 [64, 1024], P('owner', 'rows')
- serve_router: bfloat16 [2048, 64], replicated
The draws below stay inside these ranges and needn't reach their ends.
All inputs are finite; a program needn't handle non-finite values.
Results may differ from the reference program's by a relative error of at most 0.001.
Values may be sent and summed in bfloat16 or wider, within the bound.
A program may use at most 192 MiB of HBM per device.

```python
import jax
import jax.numpy as jnp
from jax import lax

EXPERTS = 64
D_MODEL = 2048
D_EXPERT = 1024


def with_spikes(values, stream_key, source, target, parts, factor):
    def block_of(position):
        return (jnp.arange(values.shape[position]) // (values.shape[position] // parts)).reshape((-1,) + (1,) * (values.ndim - 1 - position))

    near = jax.random.permutation(stream_key, parts)[block_of(target)]
    second = (block_of(target) + parts // 2) % parts
    return jnp.where((block_of(source) == near) | (block_of(source) == second), factor * values, values)


def shard_levels(rng, extent, shards, low, high):
    level = 1.0
    for axis_at, parts in shards:
        draws = jax.random.uniform(jax.random.fold_in(jax.random.fold_in(rng, 6), axis_at), (parts,), jnp.float32, low / len(shards), high / len(shards))
        level = level * jnp.repeat(jnp.exp(draws), extent[axis_at] // parts).reshape((-1,) + (1,) * (len(extent) - 1 - axis_at))
    return level


def scatter_about(stream_key, dims, scale, bound, shards=(), dtype=jnp.bfloat16):
    entries = jax.random.normal(stream_key, dims, jnp.float32) * scale
    if len(shards) > 0:
        entries = shard_levels(stream_key, dims, shards, -0.22, 0.18) * entries
    return jnp.clip(entries, min=-bound, max=bound).astype(dtype)


def noise_with(key, shape, spread, most, split, heavy, kind=jnp.bfloat16):
    array = spread * jax.random.normal(key, shape, jnp.float32)
    if split:
        array = array * shard_levels(key, shape, split, -0.22, 0.18)
    return jnp.clip(with_spikes(array, jax.random.fold_in(key, 3), *heavy), -most, most).astype(kind)


def setup_inputs(seed: int = 0) -> dict:
    key_of = jax.random.split(jax.random.key(seed), 9)
    return {
        "master_gate": noise_with(key_of[0], (EXPERTS, D_MODEL, D_EXPERT), D_MODEL ** -0.5, 0.1875, ((0, 4), (1, 8)), (1, 2, 8, 2.0), jnp.float32),
        "second_gate": scatter_about(key_of[1], (EXPERTS, D_MODEL, D_EXPERT), (D_MODEL * 4) ** -0.5, 0.0625, ((0, 4), (1, 8))),
        "master_up": noise_with(key_of[2], (EXPERTS, D_MODEL, D_EXPERT), D_MODEL ** -0.5, 0.1875, ((0, 4), (1, 8)), (1, 2, 8, 2.0), jnp.float32),
        "second_up": scatter_about(key_of[3], (EXPERTS, D_MODEL, D_EXPERT), (D_MODEL * 4) ** -0.5, 0.0625, ((0, 4), (1, 8))),
        "master_down": noise_with(key_of[4], (EXPERTS, D_EXPERT, D_MODEL), D_EXPERT ** -0.5, 0.25, ((0, 4), (2, 8)), (2, 1, 8, 2.0), jnp.float32),
        "second_down": scatter_about(key_of[5], (EXPERTS, D_EXPERT, D_MODEL), (D_EXPERT * 4) ** -0.5, 0.09375, ((0, 4), (2, 8))),
        "router_weight": scatter_about(key_of[6], (D_MODEL, EXPERTS), D_MODEL ** -0.5, 0.125, ((0, 8), (1, 4)), jnp.float32),
        "router_gain": jnp.clip(1.0 + 0.15 * jax.random.normal(key_of[7], (D_MODEL,), jnp.float32), 0.25, 1.75),
    }


def reference(master_gate, second_gate, master_up, second_up, master_down, second_down, router_weight, router_gain):
    merged_gate = master_gate + second_gate.astype(jnp.float32)
    merged_up = master_up + second_up.astype(jnp.float32)
    merged_down = master_down + second_down.astype(jnp.float32)
    scale_gate = jnp.sqrt(lax.optimization_barrier(jnp.sum(merged_gate * merged_gate, axis=1)))
    final_gate = (merged_gate / jnp.expand_dims(scale_gate, 1)).astype(jnp.bfloat16)
    scale_up = jnp.sqrt(lax.optimization_barrier(jnp.sum(merged_up * merged_up, axis=1)))
    final_up = (merged_up / jnp.expand_dims(scale_up, 1)).astype(jnp.bfloat16)
    scale_down = jnp.sqrt(lax.optimization_barrier(jnp.sum(merged_down * merged_down, axis=2)))
    final_down = (merged_down / jnp.expand_dims(scale_down, 2)).astype(jnp.bfloat16)
    serve_router = (router_weight * router_gain[:, None]).astype(jnp.bfloat16)
    return (final_gate, final_up, final_down, scale_gate, scale_up, scale_down, serve_router)
```

```python
import jax
import jax.numpy as jnp
from jax import lax
from jax.experimental import pallas as pl
from jax.experimental.pallas import tpu as pltpu
from jax.sharding import PartitionSpec as P


def narrow_kernel(master_ref, second_ref, scale_ref, out_ref):
    parts, _, _, width = out_ref.shape
    for part in range(parts):
        columns = slice(part * width, (part + 1) * width)
        merged = master_ref[0, :, columns] + second_ref[0, :, columns].astype(jnp.float32)
        out_ref[part, 0] = (merged / scale_ref[0, :, columns]).astype(jnp.bfloat16)


def narrow_columns(master, second, scale, parts):
    experts, depth, columns = master.shape
    width = columns // parts
    size = experts * depth * columns
    return pl.pallas_call(
        narrow_kernel,
        grid=(experts,),
        out_shape=jax.ShapeDtypeStruct((parts, experts, depth, width), jnp.bfloat16),
        in_specs=[
            pl.BlockSpec((1, depth, columns), lambda e: (e, 0, 0)),
            pl.BlockSpec((1, depth, columns), lambda e: (e, 0, 0)),
            pl.BlockSpec((1, 1, columns), lambda e: (e, 0, 0)),
        ],
        out_specs=pl.BlockSpec((parts, 1, depth, width), lambda e: (0, e, 0, 0)),
        compiler_params=pltpu.CompilerParams(vmem_limit_bytes=24 * 1024 * 1024),
        cost_estimate=pl.CostEstimate(flops=4 * size, bytes_accessed=8 * size, transcendentals=0),
    )(master, second, jnp.expand_dims(scale, 1))


def exchange_columns(narrow):
    parts, experts, depth, width = narrow.shape
    arrived = lax.all_to_all(narrow, "rows", split_axis=0, concat_axis=0, tiled=True)
    return arrived.transpose(1, 0, 2, 3).reshape(experts, parts * depth, width)


MESH = pl.DeviceIdType.MESH
LANES = 128
SLOTS = 3
FIRST = 6
EARLY = 3


def serve_kernel(
    master_gate,
    second_gate,
    master_up,
    second_up,
    master_down,
    second_down,
    router_weight,
    router_gain,
    final_wide,
    final_down,
    scale_gate,
    scale_up,
    scale_down,
    serve_router,
    wide_master,
    wide_second,
    tall_master,
    tall_second,
    wide_send,
    tall_send,
    first_sums,
    first_scales,
    sums,
    half_sums,
    half_total,
    other_total,
    scales,
    weight_vmem,
    gain_vmem,
    wide_sem,
    tall_sem,
    router_sem,
    bulk_sent,
    bulk_arrived,
    first_sent,
    first_arrived,
    near_sent,
    near_arrived,
    across_sent,
    across_arrived,
    back_sent,
    back_arrived,
    route_sent,
    route_arrived,
    owner_sent,
    owner_arrived,
):
    rows = lax.axis_size("rows")
    owners = lax.axis_size("owner")
    half = rows // 2
    per_rank = rows // half
    me = lax.axis_index("rows")
    owner = lax.axis_index("owner")
    rank = lax.rem(me, half)
    base = me - rank
    mirror = lax.rem(me + half, rows)
    experts, depth, _ = master_gate.shape
    width = final_wide.shape[2]
    tall = final_down.shape[1]
    across = master_down.shape[2]

    def row_peer(step):
        return lax.rem(me + step, rows)

    def half_peer(step):
        return base + lax.rem(rank + step, half)

    def owner_peer(step):
        return lax.rem(owner + step, owners)

    barrier = pltpu.get_barrier_semaphore()
    for step in range(1, rows):
        pl.semaphore_signal(barrier, inc=1, device_id={"rows": row_peer(step)}, device_id_type=MESH)
    for step in range(1, owners):
        pl.semaphore_signal(barrier, inc=1, device_id={"owner": owner_peer(step)}, device_id_type=MESH)

    def remote(source, target, sent, arrived, place):
        return pltpu.make_async_remote_copy(
            src_ref=source,
            dst_ref=target,
            send_sem=sent,
            recv_sem=arrived,
            device_id=place,
            device_id_type=MESH,
        )

    def fetch(pair, buffers, sems, expert, slot):
        return [
            pltpu.make_async_copy(pair[i].at[expert], buffers[i].at[slot], sems.at[i, slot])
            for i in range(2)
        ]

    def ahead(pair, buffers, sems, first, count):
        for i in range(min(SLOTS, count)):
            for copy in fetch(pair, buffers, sems, first + i, i):
                copy.start()

    def run(pair, buffers, sems, first, count, work):
        def step(i, _):
            slot = lax.rem(i, SLOTS)
            for copy in fetch(pair, buffers, sems, first + i, slot):
                copy.wait()
            work(first + i, slot)

            @pl.when(i + SLOTS < count)
            def _():
                for copy in fetch(pair, buffers, sems, first + i + SLOTS, slot):
                    copy.start()

            return 0

        lax.fori_loop(0, count, step, 0)

    wide = (wide_master, wide_second)
    high = (tall_master, tall_second)
    gate = (master_gate, second_gate)
    up = (master_up, second_up)
    down = (master_down, second_down)

    def wide_block(slot, part):
        columns = pl.ds(pl.multiple_of(part * width, width), width)
        return wide_master[slot, :, columns] + wide_second[slot, :, columns].astype(jnp.float32)

    def tall_block(slot, part):
        lines = pl.ds(pl.multiple_of(part * tall, tall), tall)
        return tall_master[slot, lines, :] + tall_second[slot, lines, :].astype(jnp.float32)

    def wide_total(slot, part):
        merged = wide_block(slot, part)
        return jnp.sum(merged * merged, axis=0, keepdims=True)

    def tall_total(slot, part):
        merged = tall_block(slot, part)
        square = merged * merged
        narrow = square[:, :LANES]
        for at in range(LANES, across, LANES):
            narrow = narrow + square[:, at : at + LANES]
        return jnp.sum(narrow.T, axis=0, keepdims=True)

    def sum_first(expert, slot):
        for part in range(rows):
            first_sums[me, expert, part : part + 1, :] = wide_total(slot, part)

    def sum_rest(total_of, offset):
        def work(expert, slot):
            for part in range(rows):
                sums[part, pl.ds(offset + expert, 1), :] = total_of(slot, part)

        return work

    def first_scale(expert, part):
        return first_scales[expert, pl.ds(part, 1), :]

    def rest_scale(offset):
        return lambda expert, part: scales[part, pl.ds(offset + expert, 1), :]

    my_lines = pl.ds(pl.multiple_of(me * depth, depth), depth)
    my_columns = pl.ds(pl.multiple_of(me * across, across), across)

    def narrow_wide(scale_of, which):
        def work(expert, slot):
            at = which * experts + expert

            def block(i, _):
                step = rows - 1 - i
                part = row_peer(step)
                value = wide_block(slot, part) / scale_of(expert, part)
                wide_send[at, step - 1] = value.astype(jnp.bfloat16)
                remote(
                    wide_send.at[at, step - 1],
                    final_wide.at[at, my_lines, :],
                    bulk_sent.at[which],
                    bulk_arrived.at[which],
                    {"rows": part},
                ).start()
                return 0

            lax.fori_loop(0, rows - 1, block, 0)
            own = wide_block(slot, me) / scale_of(expert, me)
            final_wide[at, my_lines, :] = own.astype(jnp.bfloat16)

        return work

    def narrow_tall(slot, part, line):
        merged = tall_block(slot, part)
        scale = jnp.broadcast_to(line, (tall, LANES)).T
        scale = jnp.concatenate([scale] * (across // LANES), axis=1)
        return (merged / scale).astype(jnp.bfloat16)

    def narrow_down(expert, slot):
        scale_of = rest_scale(2 * experts)

        def block(i, _):
            step = rows - 1 - i
            part = row_peer(step)
            tall_send[expert, step - 1] = narrow_tall(slot, part, scale_of(expert, part))
            remote(
                tall_send.at[expert, step - 1],
                final_down.at[expert, :, my_columns],
                bulk_sent.at[2],
                bulk_arrived.at[2],
                {"rows": part},
            ).start()
            return 0

        lax.fori_loop(0, rows - 1, block, 0)
        final_down[expert, :, my_columns] = narrow_tall(slot, me, scale_of(expert, me))

    ahead(gate, wide, wide_sem, 0, FIRST)
    fetch_router = [
        pltpu.make_async_copy(router_weight, weight_vmem, router_sem.at[0]),
        pltpu.make_async_copy(router_gain, gain_vmem, router_sem.at[1]),
    ]
    for copy in fetch_router:
        copy.start()
    sums[...] = jnp.zeros_like(sums)
    run(gate, wide, wide_sem, 0, FIRST, sum_first)
    ahead(gate, wide, wide_sem, 0, EARLY)
    pl.semaphore_wait(barrier, rows - 1 + owners - 1)
    first_copies = [
        remote(
            first_sums.at[me],
            first_sums.at[me],
            first_sent.at[step - 1],
            first_arrived.at[step - 1],
            {"rows": row_peer(step)},
        )
        for step in range(1, rows)
    ]
    for copy in first_copies:
        copy.start()

    for copy in fetch_router:
        copy.wait()
    mine = weight_vmem.shape[0]
    my_experts = pl.ds(pl.multiple_of(owner * mine, mine), mine)
    here = pl.ds(pl.multiple_of(me * depth, depth), depth)
    there = pl.ds(pl.multiple_of(mirror * depth, depth), depth)
    serve_router[my_experts, here] = (weight_vmem[...] * gain_vmem[...]).astype(jnp.bfloat16)
    my_route = serve_router.at[my_experts, here]
    other_route = serve_router.at[my_experts, there]
    route_copies = [remote(my_route, my_route, route_sent.at[0], route_arrived.at[0], {"rows": mirror})]
    route_copies[0].start()

    for copy in first_copies:
        copy.wait_recv()
    total = first_sums[0]
    for part in range(1, rows):
        total = total + first_sums[part]
    first_scales[...] = jnp.sqrt(total)
    narrow_first = narrow_wide(first_scale, 0)
    run(gate, wide, wide_sem, 0, EARLY, narrow_first)

    sum_gate = sum_rest(wide_total, 0)
    sum_up = sum_rest(wide_total, experts)
    sum_down = sum_rest(tall_total, 2 * experts)
    ahead(gate, wide, wide_sem, FIRST, experts - FIRST)
    ahead(down, high, tall_sem, 0, experts)
    run(gate, wide, wide_sem, FIRST, experts - FIRST, sum_gate)
    ahead(up, wide, wide_sem, 0, experts)
    run(down, high, tall_sem, 0, experts, sum_down)
    run(up, wide, wide_sem, 0, experts, sum_up)

    ahead(gate, wide, wide_sem, EARLY, 1)
    near_copies = []
    for step in range(1, half):
        peer = half_peer(step)
        peer_rank = lax.rem(rank + step, half)
        near_copies.append(
            remote(
                sums.at[pl.ds(peer_rank * per_rank, per_rank)],
                half_sums.at[rank],
                near_sent.at[step - 1],
                near_arrived.at[step - 1],
                {"rows": peer},
            )
        )
        near_copies[-1].start()
    half_sums[rank] = sums[pl.ds(rank * per_rank, per_rank)]
    run(gate, wide, wide_sem, EARLY, 1, narrow_first)
    ahead(gate, wide, wide_sem, EARLY + 1, 1)
    for copy in near_copies:
        copy.wait_recv()
    total = half_sums[0]
    for part in range(1, half):
        total = total + half_sums[part]
    half_total[...] = total
    across_copy = remote(half_total, other_total, across_sent.at[0], across_arrived.at[0], {"rows": mirror})
    across_copy.start()
    route_copies[0].wait_recv()
    for step in range(1, half):
        for i, route in enumerate((my_route, other_route)):
            at = 1 + 2 * (step - 1) + i
            route_copies.append(
                remote(route, route, route_sent.at[at], route_arrived.at[at], {"rows": half_peer(step)})
            )
            route_copies[-1].start()
    run(gate, wide, wide_sem, EARLY + 1, 1, narrow_first)
    ahead(gate, wide, wide_sem, EARLY + 2, FIRST - EARLY - 2)
    across_copy.wait_recv()
    my_parts = pl.ds(rank * per_rank, per_rank)
    scales[my_parts] = jnp.sqrt(half_total[...] + other_total[...])
    back_copies = [
        remote(
            scales.at[my_parts],
            scales.at[my_parts],
            back_sent.at[step - 1],
            back_arrived.at[step - 1],
            {"rows": half_peer(step)},
        )
        for step in range(1, half)
    ]
    for copy in back_copies:
        copy.start()
    run(gate, wide, wide_sem, EARLY + 2, FIRST - EARLY - 2, narrow_first)
    ahead(gate, wide, wide_sem, FIRST, experts - FIRST)
    ahead(down, high, tall_sem, 0, experts)
    for copy in route_copies[1:]:
        copy.wait_recv()
    owner_route = serve_router.at[my_experts, :]
    owner_copies = [
        remote(
            owner_route,
            owner_route,
            owner_sent.at[step - 1],
            owner_arrived.at[step - 1],
            {"owner": owner_peer(step)},
        )
        for step in range(1, owners)
    ]
    for copy in owner_copies:
        copy.start()
    for copy in back_copies:
        copy.wait_recv()

    run(gate, wide, wide_sem, FIRST, experts - FIRST, narrow_wide(rest_scale(0), 0))
    ahead(up, wide, wide_sem, 0, experts)
    run(up, wide, wide_sem, 0, experts, narrow_wide(rest_scale(experts), 1))
    run(down, high, tall_sem, 0, experts, narrow_down)

    scale_gate[...] = scales[me, 0:experts]
    for expert in range(FIRST):
        scale_gate[expert : expert + 1, :] = first_scale(expert, me)
    scale_up[...] = scales[me, experts : 2 * experts]
    scale_down[...] = scales[me, 2 * experts : 3 * experts]

    for copy in owner_copies:
        copy.wait_recv()
    for copies in (first_copies, route_copies, near_copies, [across_copy], back_copies, owner_copies):
        for copy in copies:
            copy.wait_send()
    incoming = pl.ds(0, (rows - 1) * depth)
    arrived = (
        final_wide.at[pl.ds(0, experts), incoming, :],
        final_wide.at[pl.ds(experts, experts), incoming, :],
        final_down.at[:, :, pl.ds(0, (rows - 1) * across)],
    )
    sent = (wide_send.at[pl.ds(0, experts)], wide_send.at[pl.ds(experts, experts)], tall_send)
    place = {"rows": row_peer(1)}
    for which in range(3):
        remote(sent[which], sent[which], bulk_sent.at[which], bulk_arrived.at[which], place).wait_send()
    for which in range(3):
        remote(arrived[which], arrived[which], bulk_sent.at[which], bulk_arrived.at[which], place).wait_recv()


def serve(
    master_gate,
    second_gate,
    master_up,
    second_up,
    master_down,
    second_down,
    router_weight,
    router_gain,
):
    rows = lax.axis_size("rows")
    owners = lax.axis_size("owner")
    half = rows // 2
    per_rank = rows // half
    experts, depth, columns = master_gate.shape
    _, lines, across = master_down.shape
    width = columns // rows
    tall = lines // rows
    mine = router_weight.shape[1]
    f32, bf16, dma = jnp.float32, jnp.bfloat16, pltpu.SemaphoreType.DMA
    chunks = 3 * experts
    hbm = pl.BlockSpec(memory_space=pltpu.HBM)
    vmem = pl.BlockSpec(memory_space=pltpu.VMEM)
    size = 3 * experts * depth * columns
    outs = pl.pallas_call(
        serve_kernel,
        out_shape=(
            pltpu.VMEM((2 * experts, rows * depth, width), bf16),
            pltpu.VMEM((experts, tall, rows * across), bf16),
            jax.ShapeDtypeStruct((experts, width), f32),
            jax.ShapeDtypeStruct((experts, width), f32),
            jax.ShapeDtypeStruct((experts, tall), f32),
            jax.ShapeDtypeStruct((owners * mine, rows * depth), bf16),
        ),
        in_specs=[hbm] * 8,
        out_specs=(vmem,) * 6,
        scratch_shapes=[
            pltpu.VMEM((SLOTS, depth, columns), f32),
            pltpu.VMEM((SLOTS, depth, columns), bf16),
            pltpu.VMEM((SLOTS, lines, across), f32),
            pltpu.VMEM((SLOTS, lines, across), bf16),
            pltpu.VMEM((2 * experts, rows - 1, depth, width), bf16),
            pltpu.VMEM((experts, rows - 1, tall, across), bf16),
            pltpu.VMEM((rows, FIRST, rows, LANES), f32),
            pltpu.VMEM((FIRST, rows, LANES), f32),
            pltpu.VMEM((rows, chunks, LANES), f32),
            pltpu.VMEM((half, per_rank, chunks, LANES), f32),
            pltpu.VMEM((per_rank, chunks, LANES), f32),
            pltpu.VMEM((per_rank, chunks, LANES), f32),
            pltpu.VMEM((rows, chunks, LANES), f32),
            pltpu.VMEM((mine, depth), f32),
            pltpu.VMEM((1, depth), f32),
            dma((2, SLOTS)),
            dma((2, SLOTS)),
            dma((2,)),
            dma((3,)),
            dma((3,)),
            dma((rows - 1,)),
            dma((rows - 1,)),
            dma((half - 1,)),
            dma((half - 1,)),
            dma((1,)),
            dma((1,)),
            dma((half - 1,)),
            dma((half - 1,)),
            dma((2 * half - 1,)),
            dma((2 * half - 1,)),
            dma((owners - 1,)),
            dma((owners - 1,)),
        ],
        compiler_params=pltpu.CompilerParams(
            collective_id=0, has_side_effects=True, vmem_limit_bytes=34 * 1024 * 1024
        ),
        cost_estimate=pl.CostEstimate(flops=8 * size, bytes_accessed=12 * size, transcendentals=0),
    )(
        master_gate,
        second_gate,
        master_up,
        second_up,
        master_down,
        second_down,
        router_weight.T,
        jnp.expand_dims(router_gain, 0),
    )
    final_gate, final_up = outs[0][:experts], outs[0][experts:]
    return (final_gate, final_up, *outs[1:5], outs[5].T)


def serve_fits(experts, depth, columns, lines, across, mine, rows):
    return (
        rows == 8
        and columns // rows == LANES
        and lines // rows == LANES
        and across % LANES == 0
        and depth % LANES == 0
        and experts % 16 == 0
        and mine % 16 == 0
        and experts > FIRST
    )


def body(
    master_gate,
    second_gate,
    master_up,
    second_up,
    master_down,
    second_down,
    router_weight,
    router_gain,
):
    parts = lax.axis_size("rows")
    if serve_fits(*master_gate.shape, *master_down.shape[1:], router_weight.shape[1], parts):
        return serve(
            master_gate,
            second_gate,
            master_up,
            second_up,
            master_down,
            second_down,
            router_weight,
            router_gain,
        )
    merged_gate = master_gate + second_gate.astype(jnp.float32)
    merged_up = master_up + second_up.astype(jnp.float32)
    merged_down = master_down + second_down.astype(jnp.float32)
    total_gate, total_up, total_down = (
        jnp.sum(lax.all_gather(part, "rows"), axis=0)
        for part in (
            jnp.sum(merged_gate * merged_gate, axis=1),
            jnp.sum(merged_up * merged_up, axis=1),
            jnp.sum(merged_down * merged_down, axis=2),
        )
    )
    part_router = (router_weight * router_gain[:, None]).astype(jnp.bfloat16)
    row_router = lax.all_gather(part_router, "rows", axis=0, tiled=True)
    serve_router = lax.all_gather(row_router, "owner", axis=1, tiled=True)
    total_gate, total_up, total_down, serve_router = lax.optimization_barrier(
        (total_gate, total_up, total_down, serve_router)
    )
    scale_gate = jnp.sqrt(total_gate)
    scale_up = jnp.sqrt(total_up)
    scale_down = jnp.sqrt(total_down)
    final_gate = exchange_columns(narrow_columns(master_gate, second_gate, scale_gate, parts))
    final_up = exchange_columns(narrow_columns(master_up, second_up, scale_up, parts))
    narrow_down = (merged_down / jnp.expand_dims(scale_down, 2)).astype(jnp.bfloat16)
    final_down = lax.all_to_all(narrow_down, "rows", split_axis=1, concat_axis=2, tiled=True)
    scale_gate = lax.dynamic_slice_in_dim(
        scale_gate, lax.axis_index("rows") * final_gate.shape[2], final_gate.shape[2], axis=1
    )
    scale_up = lax.dynamic_slice_in_dim(
        scale_up, lax.axis_index("rows") * final_up.shape[2], final_up.shape[2], axis=1
    )
    scale_down = lax.dynamic_slice_in_dim(
        scale_down, lax.axis_index("rows") * final_down.shape[1], final_down.shape[1], axis=1
    )
    return (final_gate, final_up, final_down, scale_gate, scale_up, scale_down, serve_router)


def solution(mesh):
    placed = (
        P("owner", "rows", None),
        P("owner", "rows", None),
        P("owner", "rows", None),
        P("owner", "rows", None),
        P("owner", None, "rows"),
        P("owner", None, "rows"),
        P("rows", "owner"),
        P("rows"),
    )
    return jax.shard_map(
        body,
        mesh=mesh,
        in_specs=placed,
        out_specs=(
            P("owner", None, "rows"),
            P("owner", None, "rows"),
            P("owner", "rows", None),
            P("owner", "rows"),
            P("owner", "rows"),
            P("owner", "rows"),
            P(),
        ),
        check_vma=False,
    )
```

```python
import jax
import jax.numpy as jnp
from jax import lax
from jax.experimental import pallas as pl
from jax.experimental.pallas import tpu as pltpu
from jax.sharding import PartitionSpec as P


def narrow_kernel(master_ref, second_ref, scale_ref, out_ref):
    parts, _, _, width = out_ref.shape
    for part in range(parts):
        columns = slice(part * width, (part + 1) * width)
        merged = master_ref[0, :, columns] + second_ref[0, :, columns].astype(jnp.float32)
        out_ref[part, 0] = (merged / scale_ref[0, :, columns]).astype(jnp.bfloat16)


def narrow_columns(master, second, scale, parts):
    experts, depth, columns = master.shape
    width = columns // parts
    size = experts * depth * columns
    return pl.pallas_call(
        narrow_kernel,
        grid=(experts,),
        out_shape=jax.ShapeDtypeStruct((parts, experts, depth, width), jnp.bfloat16),
        in_specs=[
            pl.BlockSpec((1, depth, columns), lambda e: (e, 0, 0)),
            pl.BlockSpec((1, depth, columns), lambda e: (e, 0, 0)),
            pl.BlockSpec((1, 1, columns), lambda e: (e, 0, 0)),
        ],
        out_specs=pl.BlockSpec((parts, 1, depth, width), lambda e: (0, e, 0, 0)),
        compiler_params=pltpu.CompilerParams(vmem_limit_bytes=24 * 1024 * 1024),
        cost_estimate=pl.CostEstimate(flops=4 * size, bytes_accessed=8 * size, transcendentals=0),
    )(master, second, jnp.expand_dims(scale, 1))


def exchange_columns(narrow):
    parts, experts, depth, width = narrow.shape
    arrived = lax.all_to_all(narrow, "rows", split_axis=0, concat_axis=0, tiled=True)
    return arrived.transpose(1, 0, 2, 3).reshape(experts, parts * depth, width)


MESH = pl.DeviceIdType.MESH
LANES = 128
SLOTS = 3
FIRST = 2
FILL = 2


def serve_kernel(
    master_gate,
    second_gate,
    master_up,
    second_up,
    master_down,
    second_down,
    router_weight,
    router_gain,
    final_wide,
    final_down,
    scale_all,
    serve_router,
    held_master,
    held_second,
    wide_master,
    wide_second,
    tall_master,
    tall_second,
    wide_send,
    tall_send,
    first_sums,
    first_scales,
    sums,
    half_sums,
    half_total,
    other_total,
    scales,
    weight_vmem,
    gain_vmem,
    held_sem,
    wide_sem,
    tall_sem,
    router_sem,
    bulk_sent,
    bulk_arrived,
    first_sent,
    first_arrived,
    near_sent,
    near_arrived,
    across_sent,
    across_arrived,
    back_sent,
    back_arrived,
    route_sent,
    route_arrived,
    owner_sent,
    owner_arrived,
):
    rows = lax.axis_size("rows")
    owners = lax.axis_size("owner")
    half = rows // 2
    per_rank = rows // half
    me = lax.axis_index("rows")
    owner = lax.axis_index("owner")
    rank = lax.rem(me, half)
    base = me - rank
    mirror = lax.rem(me + half, rows)
    experts, depth, _ = master_gate.shape
    width = final_wide.shape[2]
    tall = final_down.shape[1]
    across = master_down.shape[2]
    sent_copies = []

    def row_peer(step):
        return lax.rem(me + step, rows)

    def half_peer(step):
        return base + lax.rem(rank + step, half)

    def owner_peer(step):
        return lax.rem(owner + step, owners)

    barrier = pltpu.get_barrier_semaphore()
    for step in range(1, rows):
        pl.semaphore_signal(barrier, inc=1, device_id={"rows": row_peer(step)}, device_id_type=MESH)
    for step in range(1, owners):
        pl.semaphore_signal(barrier, inc=1, device_id={"owner": owner_peer(step)}, device_id_type=MESH)

    def remote(source, target, sent, arrived, place):
        return pltpu.make_async_remote_copy(
            src_ref=source,
            dst_ref=target,
            send_sem=sent,
            recv_sem=arrived,
            device_id=place,
            device_id_type=MESH,
        )

    def post(source, target, sent, arrived, place):
        copy = remote(source, target, sent, arrived, place)
        copy.start()
        sent_copies.append(copy)
        return copy

    def fetch(pair, buffers, sems, expert, slot):
        return [
            pltpu.make_async_copy(pair[i].at[expert], buffers[i].at[slot], sems.at[i, slot])
            for i in range(2)
        ]

    class Stream:
        def __init__(self, pair, buffers, sems, first, last):
            self.pair, self.buffers, self.sems = pair, buffers, sems
            self.first, self.last = first, last
            for i in range(min(SLOTS, last - first)):
                for copy in fetch(pair, buffers, sems, first + i, i):
                    copy.start()

        def run(self, begin, end, work):
            def step(expert, _):
                slot = lax.rem(expert - self.first, SLOTS)
                for copy in fetch(self.pair, self.buffers, self.sems, expert, slot):
                    copy.wait()
                work(expert, slot)

                @pl.when(expert + SLOTS < self.last)
                def _():
                    for copy in fetch(self.pair, self.buffers, self.sems, expert + SLOTS, slot):
                        copy.start()

                return 0

            lax.fori_loop(begin, end, step, 0)

    held = (held_master, held_second)
    wide = (wide_master, wide_second)
    high = (tall_master, tall_second)
    gate = (master_gate, second_gate)
    up = (master_up, second_up)
    down = (master_down, second_down)

    def wide_block(buffers, slot, part):
        columns = pl.ds(pl.multiple_of(part * width, width), width)
        return buffers[0][slot, :, columns] + buffers[1][slot, :, columns].astype(jnp.float32)

    def tall_block(slot, part):
        lines = pl.ds(pl.multiple_of(part * tall, tall), tall)
        return tall_master[slot, lines, :] + tall_second[slot, lines, :].astype(jnp.float32)

    def wide_total(slot, part, buffers=wide):
        merged = wide_block(buffers, slot, part)
        return jnp.sum(merged * merged, axis=0, keepdims=True)

    def tall_total(slot, part):
        merged = tall_block(slot, part)
        square = merged * merged
        narrow = square[:, :LANES]
        for at in range(LANES, across, LANES):
            narrow = narrow + square[:, at : at + LANES]
        return jnp.sum(narrow.T, axis=0, keepdims=True)

    def sum_rest(total_of, offset):
        def work(expert, slot):
            for part in range(rows):
                sums[part, pl.ds(offset + expert, 1), :] = total_of(slot, part)

        return work

    def first_scale(expert, part):
        return first_scales[expert, pl.ds(part, 1), :]

    def rest_scale(offset):
        return lambda expert, part: scales[part, pl.ds(offset + expert, 1), :]

    my_lines = pl.ds(pl.multiple_of(me * depth, depth), depth)
    my_columns = pl.ds(pl.multiple_of(me * across, across), across)

    def part_of(slot):
        part, bit = 0, 1
        while bit < rows:
            part = part + bit * lax.rem(me // bit + 1 + slot // bit, 2)
            bit = 2 * bit
        return part

    def narrow_wide(scale_of, which, buffers=wide, begin=0, end=rows - 1):
        def work(expert, slot):
            at = which * experts + expert

            def block(i, _):
                part = part_of(i)
                value = wide_block(buffers, slot, part) / scale_of(expert, part)
                wide_send[at, i] = value.astype(jnp.bfloat16)
                remote(
                    wide_send.at[at, i],
                    final_wide.at[at, my_lines, :],
                    bulk_sent.at[which],
                    bulk_arrived.at[which],
                    {"rows": part},
                ).start()
                return 0

            lax.fori_loop(begin, end, block, 0)
            if end == rows - 1:
                own = wide_block(buffers, slot, me) / scale_of(expert, me)
                final_wide[at, my_lines, :] = own.astype(jnp.bfloat16)

        return work

    def narrow_tall(slot, part, line):
        merged = tall_block(slot, part)
        scale = jnp.broadcast_to(line, (tall, LANES)).T
        scale = jnp.concatenate([scale] * (across // LANES), axis=1)
        return (merged / scale).astype(jnp.bfloat16)

    def narrow_down(expert, slot):
        scale_of = rest_scale(2 * experts)

        def block(i, _):
            part = part_of(i)
            tall_send[expert, i] = narrow_tall(slot, part, scale_of(expert, part))
            remote(
                tall_send.at[expert, i],
                final_down.at[expert, :, my_columns],
                bulk_sent.at[2],
                bulk_arrived.at[2],
                {"rows": part},
            ).start()
            return 0

        lax.fori_loop(0, rows - 1, block, 0)
        final_down[expert, :, my_columns] = narrow_tall(slot, me, scale_of(expert, me))

    my_parts = pl.ds(rank * per_rank, per_rank)

    def send_near(which, lines):
        copies = []
        for step in range(1, half):
            parts = pl.ds(lax.rem(rank + step, half) * per_rank, per_rank)
            copies.append(
                post(
                    sums.at[parts, lines],
                    half_sums.at[rank, :, lines],
                    near_sent.at[which, step - 1],
                    near_arrived.at[which, step - 1],
                    {"rows": half_peer(step)},
                )
            )
        half_sums[rank, :, lines] = sums[my_parts, lines]
        return copies

    def send_across(which, lines, copies):
        for copy in copies:
            copy.wait_recv()
        total = half_sums[0, :, lines]
        for part in range(1, half):
            total = total + half_sums[part, :, lines]
        half_total[:, lines] = total
        return post(
            half_total.at[:, lines],
            other_total.at[:, lines],
            across_sent.at[which],
            across_arrived.at[which],
            {"rows": mirror},
        )

    def send_back(which, lines, copy):
        copy.wait_recv()
        scales[my_parts, lines] = jnp.sqrt(half_total[:, lines] + other_total[:, lines])
        place = scales.at[my_parts, lines]
        return [
            post(
                place,
                place,
                back_sent.at[which, step - 1],
                back_arrived.at[which, step - 1],
                {"rows": half_peer(step)},
            )
            for step in range(1, half)
        ]

    for expert in range(FIRST):
        for copy in fetch(gate, held, held_sem, expert, expert):
            copy.start()
    stream = Stream(gate, wide, wide_sem, FIRST, experts)
    fetch_router = [
        pltpu.make_async_copy(router_weight, weight_vmem, router_sem.at[0]),
        pltpu.make_async_copy(router_gain, gain_vmem, router_sem.at[1]),
    ]
    for copy in fetch_router:
        copy.start()
    for part in range(rows):
        sums[part, 0:8, :] = jnp.zeros((8, LANES), jnp.float32)
    for expert in range(FIRST):
        for copy in fetch(gate, held, held_sem, expert, expert):
            copy.wait()
        for part in range(rows):
            first_sums[me, expert, part : part + 1, :] = wide_total(expert, part, held)
    pl.semaphore_wait(barrier, rows - 1 + owners - 1)
    first_copies = [
        post(
            first_sums.at[me],
            first_sums.at[me],
            first_sent.at[step - 1],
            first_arrived.at[step - 1],
            {"rows": row_peer(step)},
        )
        for step in range(1, rows)
    ]
    sum_gate = sum_rest(wide_total, 0)
    stream.run(FIRST, FIRST + FILL, sum_gate)
    for copy in first_copies:
        copy.wait_recv()
    total = first_sums[0]
    for part in range(1, rows):
        total = total + first_sums[part]
    first_scales[...] = jnp.sqrt(total)

    middle = rows // 2
    early = narrow_wide(first_scale, 0, held, 0, middle)
    late = narrow_wide(first_scale, 0, held, middle, rows - 1)
    lines = pl.ds(0, experts)
    early(0, 0)
    stream.run(FIRST + FILL, experts, sum_gate)
    copies = send_near(0, lines)
    late(0, 0)
    near_end = experts // 2
    stream = Stream(gate, wide, wide_sem, FIRST, near_end)
    copy = send_across(0, lines, copies)
    for expert in range(1, FIRST - 1):
        early(expert, expert)
        late(expert, expert)
    early(FIRST - 1, FIRST - 1)
    copies = send_back(0, lines, copy)
    late(FIRST - 1, FIRST - 1)

    for copy in fetch_router:
        copy.wait()
    mine = weight_vmem.shape[0]
    my_experts = pl.ds(pl.multiple_of(owner * mine, mine), mine)
    here = pl.ds(pl.multiple_of(me * depth, depth), depth)
    there = pl.ds(pl.multiple_of(mirror * depth, depth), depth)
    serve_router[my_experts, here] = (weight_vmem[...] * gain_vmem[...]).astype(jnp.bfloat16)
    my_route = serve_router.at[my_experts, here]
    other_route = serve_router.at[my_experts, there]
    mirrored = post(my_route, my_route, route_sent.at[0], route_arrived.at[0], {"rows": mirror})

    for copy in copies:
        copy.wait_recv()
    narrow_gate = narrow_wide(rest_scale(0), 0)
    stream.run(FIRST, near_end, narrow_gate)

    stream = Stream(up, wide, wide_sem, 0, experts)
    other = Stream(down, high, tall_sem, 0, experts)
    stream.run(0, experts, sum_rest(wide_total, experts))
    stream = Stream(gate, wide, wide_sem, near_end, experts)
    other.run(0, experts, sum_rest(tall_total, 2 * experts))
    other = Stream(down, high, tall_sem, 0, experts)
    lines = pl.ds(experts, 2 * experts)
    copies = send_near(1, lines)
    stream.run(near_end, near_end + 2, narrow_gate)
    copy = send_across(1, lines, copies)
    mirrored.wait_recv()
    routes = []
    for step in range(1, half):
        for i, route in enumerate((my_route, other_route)):
            at = 1 + 2 * (step - 1) + i
            routes.append(
                post(route, route, route_sent.at[at], route_arrived.at[at], {"rows": half_peer(step)})
            )
    stream.run(near_end + 2, near_end + 4, narrow_gate)
    copies = send_back(1, lines, copy)
    for copy in routes:
        copy.wait_recv()
    owner_route = serve_router.at[my_experts, :]
    owner_copies = [
        post(
            owner_route,
            owner_route,
            owner_sent.at[step - 1],
            owner_arrived.at[step - 1],
            {"owner": owner_peer(step)},
        )
        for step in range(1, owners)
    ]
    stream.run(near_end + 4, experts, narrow_gate)
    stream = Stream(up, wide, wide_sem, 0, experts)
    for copy in copies:
        copy.wait_recv()

    stream.run(0, experts, narrow_wide(rest_scale(experts), 1))
    other.run(0, experts, narrow_down)

    for which in range(3):
        scale_all[which] = scales[me, which * experts : (which + 1) * experts]
    for expert in range(FIRST):
        scale_all[0, expert : expert + 1, :] = first_scale(expert, me)

    for copy in owner_copies:
        copy.wait_recv()
    for copy in sent_copies:
        copy.wait_send()
    incoming = pl.ds(0, (rows - 1) * depth)
    arrived = (
        final_wide.at[pl.ds(0, experts), incoming, :],
        final_wide.at[pl.ds(experts, experts), incoming, :],
        final_down.at[:, :, pl.ds(0, (rows - 1) * across)],
    )
    sent = (wide_send.at[pl.ds(0, experts)], wide_send.at[pl.ds(experts, experts)], tall_send)
    place = {"rows": row_peer(1)}
    for which in range(3):
        remote(sent[which], sent[which], bulk_sent.at[which], bulk_arrived.at[which], place).wait_send()
    for which in range(3):
        remote(arrived[which], arrived[which], bulk_sent.at[which], bulk_arrived.at[which], place).wait_recv()


def deliver_kernel(wide, down, scale_all, router, gate_out, up_out, down_out, *rest):
    scale_outs, router_out, sems = rest[:3], rest[3], rest[4]
    experts = gate_out.shape[0]
    pairs = [
        (wide.at[pl.ds(0, experts)], gate_out),
        (wide.at[pl.ds(experts, experts)], up_out),
        (down, down_out),
        (router, router_out),
    ]
    pairs += [(scale_all.at[i], scale_outs[i]) for i in range(3)]
    copies = [pltpu.make_async_copy(*pair, sems.at[i]) for i, pair in enumerate(pairs)]
    for copy in copies:
        copy.start()
    for copy in copies:
        copy.wait()


def serve(
    master_gate,
    second_gate,
    master_up,
    second_up,
    master_down,
    second_down,
    router_weight,
    router_gain,
):
    rows = lax.axis_size("rows")
    owners = lax.axis_size("owner")
    half = rows // 2
    per_rank = rows // half
    experts, depth, columns = master_gate.shape
    _, lines, across = master_down.shape
    width = columns // rows
    tall = lines // rows
    mine = router_weight.shape[1]
    f32, bf16, dma = jnp.float32, jnp.bfloat16, pltpu.SemaphoreType.DMA
    chunks = 3 * experts
    hbm = pl.BlockSpec(memory_space=pltpu.HBM)
    vmem = pl.BlockSpec(memory_space=pltpu.VMEM)
    size = 3 * experts * depth * columns
    arrived = pl.pallas_call(
        serve_kernel,
        out_shape=(
            pltpu.VMEM((2 * experts, rows * depth, width), bf16),
            pltpu.VMEM((experts, tall, rows * across), bf16),
            pltpu.VMEM((3, experts, width), f32),
            pltpu.VMEM((owners * mine, rows * depth), bf16),
        ),
        in_specs=[hbm] * 8,
        out_specs=(vmem,) * 4,
        scratch_shapes=[
            pltpu.VMEM((FIRST, depth, columns), f32),
            pltpu.VMEM((FIRST, depth, columns), bf16),
            pltpu.VMEM((SLOTS, depth, columns), f32),
            pltpu.VMEM((SLOTS, depth, columns), bf16),
            pltpu.VMEM((SLOTS, lines, across), f32),
            pltpu.VMEM((SLOTS, lines, across), bf16),
            pltpu.VMEM((2 * experts, rows - 1, depth, width), bf16),
            pltpu.VMEM((experts, rows - 1, tall, across), bf16),
            pltpu.VMEM((rows, FIRST, rows, LANES), f32),
            pltpu.VMEM((FIRST, rows, LANES), f32),
            pltpu.VMEM((rows, chunks, LANES), f32),
            pltpu.VMEM((half, per_rank, chunks, LANES), f32),
            pltpu.VMEM((per_rank, chunks, LANES), f32),
            pltpu.VMEM((per_rank, chunks, LANES), f32),
            pltpu.VMEM((rows, chunks, LANES), f32),
            pltpu.VMEM((mine, depth), f32),
            pltpu.VMEM((1, depth), f32),
            dma((2, FIRST)),
            dma((2, SLOTS)),
            dma((2, SLOTS)),
            dma((2,)),
            dma((3,)),
            dma((3,)),
            dma((rows - 1,)),
            dma((rows - 1,)),
            dma((2, half - 1)),
            dma((2, half - 1)),
            dma((2,)),
            dma((2,)),
            dma((2, half - 1)),
            dma((2, half - 1)),
            dma((2 * half - 1,)),
            dma((2 * half - 1,)),
            dma((owners - 1,)),
            dma((owners - 1,)),
        ],
        compiler_params=pltpu.CompilerParams(
            collective_id=0, has_side_effects=True, vmem_limit_bytes=36 * 1024 * 1024
        ),
        cost_estimate=pl.CostEstimate(flops=8 * size, bytes_accessed=12 * size, transcendentals=0),
    )(
        master_gate,
        second_gate,
        master_up,
        second_up,
        master_down,
        second_down,
        router_weight.T,
        jnp.expand_dims(router_gain, 0),
    )
    outs = pl.pallas_call(
        deliver_kernel,
        out_shape=(
            jax.ShapeDtypeStruct((experts, rows * depth, width), bf16),
            jax.ShapeDtypeStruct((experts, rows * depth, width), bf16),
            jax.ShapeDtypeStruct((experts, tall, rows * across), bf16),
            jax.ShapeDtypeStruct((experts, width), f32),
            jax.ShapeDtypeStruct((experts, width), f32),
            jax.ShapeDtypeStruct((experts, tall), f32),
            jax.ShapeDtypeStruct((owners * mine, rows * depth), bf16),
        ),
        in_specs=[vmem] * 4,
        out_specs=(hbm,) * 7,
        scratch_shapes=[dma((7,))],
        compiler_params=pltpu.CompilerParams(vmem_limit_bytes=2 * 1024 * 1024),
        cost_estimate=pl.CostEstimate(flops=size, bytes_accessed=4 * size, transcendentals=0),
    )(*arrived)
    return (*outs[:6], outs[6].T)


def serve_fits(experts, depth, columns, lines, across, mine, rows):
    return (
        rows == 8
        and columns // rows == LANES
        and lines // rows == LANES
        and across % LANES == 0
        and depth % LANES == 0
        and experts % 16 == 0
        and mine % 16 == 0
        and experts >= FIRST + FILL
    )


def body(
    master_gate,
    second_gate,
    master_up,
    second_up,
    master_down,
    second_down,
    router_weight,
    router_gain,
):
    parts = lax.axis_size("rows")
    if serve_fits(*master_gate.shape, *master_down.shape[1:], router_weight.shape[1], parts):
        return serve(
            master_gate,
            second_gate,
            master_up,
            second_up,
            master_down,
            second_down,
            router_weight,
            router_gain,
        )
    merged_gate = master_gate + second_gate.astype(jnp.float32)
    merged_up = master_up + second_up.astype(jnp.float32)
    merged_down = master_down + second_down.astype(jnp.float32)
    total_gate, total_up, total_down = (
        jnp.sum(lax.all_gather(part, "rows"), axis=0)
        for part in (
            jnp.sum(merged_gate * merged_gate, axis=1),
            jnp.sum(merged_up * merged_up, axis=1),
            jnp.sum(merged_down * merged_down, axis=2),
        )
    )
    part_router = (router_weight * router_gain[:, None]).astype(jnp.bfloat16)
    row_router = lax.all_gather(part_router, "rows", axis=0, tiled=True)
    serve_router = lax.all_gather(row_router, "owner", axis=1, tiled=True)
    total_gate, total_up, total_down, serve_router = lax.optimization_barrier(
        (total_gate, total_up, total_down, serve_router)
    )
    scale_gate = jnp.sqrt(total_gate)
    scale_up = jnp.sqrt(total_up)
    scale_down = jnp.sqrt(total_down)
    final_gate = exchange_columns(narrow_columns(master_gate, second_gate, scale_gate, parts))
    final_up = exchange_columns(narrow_columns(master_up, second_up, scale_up, parts))
    narrow_down = (merged_down / jnp.expand_dims(scale_down, 2)).astype(jnp.bfloat16)
    final_down = lax.all_to_all(narrow_down, "rows", split_axis=1, concat_axis=2, tiled=True)
    scale_gate = lax.dynamic_slice_in_dim(
        scale_gate, lax.axis_index("rows") * final_gate.shape[2], final_gate.shape[2], axis=1
    )
    scale_up = lax.dynamic_slice_in_dim(
        scale_up, lax.axis_index("rows") * final_up.shape[2], final_up.shape[2], axis=1
    )
    scale_down = lax.dynamic_slice_in_dim(
        scale_down, lax.axis_index("rows") * final_down.shape[1], final_down.shape[1], axis=1
    )
    return (final_gate, final_up, final_down, scale_gate, scale_up, scale_down, serve_router)


def solution(mesh):
    placed = (
        P("owner", "rows", None),
        P("owner", "rows", None),
        P("owner", "rows", None),
        P("owner", "rows", None),
        P("owner", None, "rows"),
        P("owner", None, "rows"),
        P("rows", "owner"),
        P("rows"),
    )
    return jax.shard_map(
        body,
        mesh=mesh,
        in_specs=placed,
        out_specs=(
            P("owner", None, "rows"),
            P("owner", None, "rows"),
            P("owner", "rows", None),
            P("owner", "rows"),
            P("owner", "rows"),
            P("owner", "rows"),
            P(),
        ),
        check_vma=False,
    )
```

```python
import functools

import jax
import jax.numpy as jnp
from jax import lax
from jax.experimental import pallas as pl
from jax.experimental.pallas import tpu as pltpu
from jax.sharding import PartitionSpec as P


def narrow_kernel(master_ref, second_ref, scale_ref, out_ref):
    parts, _, _, width = out_ref.shape
    for part in range(parts):
        columns = slice(part * width, (part + 1) * width)
        merged = master_ref[0, :, columns] + second_ref[0, :, columns].astype(jnp.float32)
        out_ref[part, 0] = (merged / scale_ref[0, :, columns]).astype(jnp.bfloat16)


def narrow_columns(master, second, scale, parts):
    experts, depth, columns = master.shape
    width = columns // parts
    size = experts * depth * columns
    return pl.pallas_call(
        narrow_kernel,
        grid=(experts,),
        out_shape=jax.ShapeDtypeStruct((parts, experts, depth, width), jnp.bfloat16),
        in_specs=[
            pl.BlockSpec((1, depth, columns), lambda e: (e, 0, 0)),
            pl.BlockSpec((1, depth, columns), lambda e: (e, 0, 0)),
            pl.BlockSpec((1, 1, columns), lambda e: (e, 0, 0)),
        ],
        out_specs=pl.BlockSpec((parts, 1, depth, width), lambda e: (0, e, 0, 0)),
        compiler_params=pltpu.CompilerParams(vmem_limit_bytes=24 * 1024 * 1024),
        cost_estimate=pl.CostEstimate(flops=4 * size, bytes_accessed=8 * size, transcendentals=0),
    )(master, second, jnp.expand_dims(scale, 1))


def exchange_columns(narrow):
    parts, experts, depth, width = narrow.shape
    arrived = lax.all_to_all(narrow, "rows", split_axis=0, concat_axis=0, tiled=True)
    return arrived.transpose(1, 0, 2, 3).reshape(experts, parts * depth, width)


MESH = pl.DeviceIdType.MESH
LANES = 128
SLOTS = 3
FIRST = 2
SECOND = 8
PIECES = 4


def serve_kernel(
    master_gate,
    second_gate,
    master_up,
    second_up,
    master_down,
    second_down,
    router_weight,
    router_gain,
    final_wide,
    final_down,
    scale_all,
    serve_router,
    held_master,
    held_second,
    wide_master,
    wide_second,
    tall_master,
    tall_second,
    wide_send,
    tall_send,
    first_sums,
    first_scales,
    sums,
    half_sums,
    half_total,
    other_total,
    scales,
    weight_vmem,
    gain_vmem,
    held_sem,
    wide_sem,
    tall_sem,
    router_sem,
    bulk_sent,
    bulk_arrived,
    first_sent,
    first_arrived,
    near_sent,
    near_arrived,
    across_sent,
    across_arrived,
    back_sent,
    back_arrived,
    route_sent,
    route_arrived,
    owner_sent,
    owner_arrived,
):
    rows = lax.axis_size("rows")
    owners = lax.axis_size("owner")
    half = rows // 2
    per_rank = rows // half
    me = lax.axis_index("rows")
    owner = lax.axis_index("owner")
    rank = lax.rem(me, half)
    base = me - rank
    mirror = lax.rem(me + half, rows)
    experts, depth, _ = master_gate.shape
    width = final_wide.shape[2]
    tall = final_down.shape[1]
    across = master_down.shape[2]
    sent_copies = []

    def row_peer(step):
        return lax.rem(me + step, rows)

    def half_peer(step):
        return base + lax.rem(rank + step, half)

    def owner_peer(step):
        return lax.rem(owner + step, owners)

    barrier = pltpu.get_barrier_semaphore()
    for step in range(1, rows):
        pl.semaphore_signal(barrier, inc=1, device_id={"rows": row_peer(step)}, device_id_type=MESH)
    for step in range(1, owners):
        pl.semaphore_signal(barrier, inc=1, device_id={"owner": owner_peer(step)}, device_id_type=MESH)

    def remote(source, target, sent, arrived, place):
        return pltpu.make_async_remote_copy(
            src_ref=source,
            dst_ref=target,
            send_sem=sent,
            recv_sem=arrived,
            device_id=place,
            device_id_type=MESH,
        )

    def post(source, target, sent, arrived, place):
        copy = remote(source, target, sent, arrived, place)
        copy.start()
        sent_copies.append(copy)
        return copy

    def fetch(pair, buffers, sems, expert, slot):
        return [
            pltpu.make_async_copy(pair[i].at[expert], buffers[i].at[slot], sems.at[i, slot])
            for i in range(2)
        ]

    class Stream:
        def __init__(self, pair, buffers, sems, first, last):
            self.pair, self.buffers, self.sems = pair, buffers, sems
            self.first, self.last = first, last
            for i in range(min(SLOTS, last - first)):
                for copy in fetch(pair, buffers, sems, first + i, i):
                    copy.start()

        def run(self, begin, end, work):
            def step(expert, _):
                slot = lax.rem(expert - self.first, SLOTS)
                for copy in fetch(self.pair, self.buffers, self.sems, expert, slot):
                    copy.wait()
                work(expert, slot)

                @pl.when(expert + SLOTS < self.last)
                def _():
                    for copy in fetch(self.pair, self.buffers, self.sems, expert + SLOTS, slot):
                        copy.start()

                return 0

            lax.fori_loop(begin, end, step, 0)

    held = (held_master, held_second)
    wide = (wide_master, wide_second)
    high = (tall_master, tall_second)
    gate = (master_gate, second_gate)
    up = (master_up, second_up)
    down = (master_down, second_down)

    def wide_block(buffers, slot, part):
        columns = pl.ds(pl.multiple_of(part * width, width), width)
        return buffers[0][slot, :, columns] + buffers[1][slot, :, columns].astype(jnp.float32)

    def tall_block(slot, part):
        lines = pl.ds(pl.multiple_of(part * tall, tall), tall)
        return tall_master[slot, lines, :] + tall_second[slot, lines, :].astype(jnp.float32)

    def wide_total(slot, part, buffers=wide):
        merged = wide_block(buffers, slot, part)
        return jnp.sum(merged * merged, axis=0, keepdims=True)

    def tall_total(slot, part):
        merged = tall_block(slot, part)
        square = merged * merged
        narrow = square[:, :LANES]
        for at in range(LANES, across, LANES):
            narrow = narrow + square[:, at : at + LANES]
        return jnp.sum(narrow.T, axis=0, keepdims=True)

    def sum_rest(total_of, offset):
        def work(expert, slot):
            for part in range(rows):
                sums[part, pl.ds(offset + expert, 1), :] = total_of(slot, part)

        return work

    def first_scale(expert, part):
        return first_scales[expert, pl.ds(part, 1), :]

    def rest_scale(offset):
        return lambda expert, part: scales[part, pl.ds(offset + expert, 1), :]

    my_lines = pl.ds(pl.multiple_of(me * depth, depth), depth)
    my_columns = pl.ds(pl.multiple_of(me * across, across), across)

    def part_of(slot):
        part, bit = 0, 1
        while bit < rows:
            part = part + bit * lax.rem(me // bit + 1 + slot // bit, 2)
            bit = 2 * bit
        return part

    def last_part_of(slot):
        across_part = lax.rem(base + half, rows) + slot
        return jnp.where(slot < half, across_part, base + lax.rem(rank + slot + 1, half))

    def narrow_wide(scale_of, which, buffers=wide, begin=0, end=rows - 1):
        def work(expert, slot):
            at = which * experts + expert

            def block(i, _):
                part = part_of(i)
                value = wide_block(buffers, slot, part) / scale_of(expert, part)
                wide_send[at, i] = value.astype(jnp.bfloat16)
                remote(
                    wide_send.at[at, i],
                    final_wide.at[at, my_lines, :],
                    bulk_sent.at[which],
                    bulk_arrived.at[which],
                    {"rows": part},
                ).start()
                return 0

            lax.fori_loop(begin, end, block, 0)
            if end == rows - 1:
                own = wide_block(buffers, slot, me) / scale_of(expert, me)
                final_wide[at, my_lines, :] = own.astype(jnp.bfloat16)

        return work

    def narrow_tall(slot, part, line):
        merged = tall_block(slot, part)
        scale = jnp.broadcast_to(line, (tall, LANES)).T
        scale = jnp.concatenate([scale] * (across // LANES), axis=1)
        return (merged / scale).astype(jnp.bfloat16)

    def narrow_down(expert, slot, part_at=part_of):
        scale_of = rest_scale(2 * experts)

        def block(i, _):
            part = part_at(i)
            tall_send[expert, i] = narrow_tall(slot, part, scale_of(expert, part))
            remote(
                tall_send.at[expert, i],
                final_down.at[expert, :, my_columns],
                bulk_sent.at[2],
                bulk_arrived.at[2],
                {"rows": part},
            ).start()
            return 0

        lax.fori_loop(0, rows - 1, block, 0)
        final_down[expert, :, my_columns] = narrow_tall(slot, me, scale_of(expert, me))

    my_parts = pl.ds(rank * per_rank, per_rank)

    def send_near(which, lines):
        copies = []
        for step in range(1, half):
            parts = pl.ds(lax.rem(rank + step, half) * per_rank, per_rank)
            copies.append(
                post(
                    sums.at[parts, lines],
                    half_sums.at[rank, :, lines],
                    near_sent.at[which, step - 1],
                    near_arrived.at[which, step - 1],
                    {"rows": half_peer(step)},
                )
            )
        half_sums[rank, :, lines] = sums[my_parts, lines]
        return copies

    def send_across(which, lines, copies):
        for copy in copies:
            copy.wait_recv()
        total = half_sums[0, :, lines]
        for part in range(1, half):
            total = total + half_sums[part, :, lines]
        half_total[:, lines] = total
        return post(
            half_total.at[:, lines],
            other_total.at[:, lines],
            across_sent.at[which],
            across_arrived.at[which],
            {"rows": mirror},
        )

    def send_back(which, lines, copy):
        copy.wait_recv()
        scales[my_parts, lines] = jnp.sqrt(half_total[:, lines] + other_total[:, lines])
        place = scales.at[my_parts, lines]
        return [
            post(
                place,
                place,
                back_sent.at[which, step - 1],
                back_arrived.at[which, step - 1],
                {"rows": half_peer(step)},
            )
            for step in range(1, half)
        ]

    for expert in range(FIRST):
        for copy in fetch(gate, held, held_sem, expert, expert):
            copy.start()
    fetch_router = [
        pltpu.make_async_copy(router_weight, weight_vmem, router_sem.at[0]),
        pltpu.make_async_copy(router_gain, gain_vmem, router_sem.at[1]),
    ]
    for copy in fetch_router:
        copy.start()
    for part in range(rows):
        sums[part, 0:8, :] = jnp.zeros((8, LANES), jnp.float32)
    first_copies = []
    for expert in range(FIRST):
        for copy in fetch(gate, held, held_sem, expert, expert):
            copy.wait()
        for part in range(rows):
            first_sums[me, expert, part : part + 1, :] = wide_total(expert, part, held)
        if expert == 0:
            pl.semaphore_wait(barrier, rows - 1 + owners - 1)
        first_copies.append(
            [
                post(
                    first_sums.at[me, expert],
                    first_sums.at[me, expert],
                    first_sent.at[expert, step - 1],
                    first_arrived.at[expert, step - 1],
                    {"rows": row_peer(step)},
                )
                for step in range(1, rows)
            ]
        )

    for copy in fetch_router:
        copy.wait()
    mine = weight_vmem.shape[0]
    my_experts = pl.ds(pl.multiple_of(owner * mine, mine), mine)
    here = pl.ds(pl.multiple_of(me * depth, depth), depth)
    there = pl.ds(pl.multiple_of(mirror * depth, depth), depth)
    serve_router[my_experts, here] = (weight_vmem[...] * gain_vmem[...]).astype(jnp.bfloat16)
    my_route = serve_router.at[my_experts, here]
    other_route = serve_router.at[my_experts, there]
    mirrored = post(my_route, my_route, route_sent.at[0], route_arrived.at[0], {"rows": mirror})

    stream = Stream(gate, wide, wide_sem, FIRST, SECOND)
    sum_gate = sum_rest(wide_total, 0)
    def total_first(expert):
        for copy in first_copies[expert]:
            copy.wait_recv()
        total = first_sums[0, expert]
        for part in range(1, rows):
            total = total + first_sums[part, expert]
        first_scales[expert] = jnp.sqrt(total)

    def piece(expert, begin, end):
        narrow_wide(first_scale, 0, held, begin, end)(expert, expert)

    total_first(0)
    piece(0, 0, half // 2)
    stream.run(FIRST, SECOND, sum_gate)
    lines = pl.ds(0, SECOND)
    copies = send_near(0, lines)
    stream = Stream(gate, wide, wide_sem, FIRST, SECOND - 3)
    piece(0, half // 2, half)
    copy = send_across(0, lines, copies)
    total_first(1)
    piece(1, 0, half // 2)
    copies = send_back(0, lines, copy)
    piece(0, half, rows - 1)
    piece(1, half // 2, rows - 1)

    for copy in copies:
        copy.wait_recv()
    narrow_gate = narrow_wide(rest_scale(0), 0)
    stream.run(FIRST, SECOND - 3, narrow_gate)

    stream = Stream(gate, wide, wide_sem, SECOND, experts)
    other = Stream(down, high, tall_sem, 0, experts)
    stream.run(SECOND, experts, sum_gate)
    stream = Stream(up, wide, wide_sem, 0, experts)
    other.run(0, experts, sum_rest(tall_total, 2 * experts))
    other = Stream(down, high, tall_sem, 0, experts)
    stream.run(0, experts, sum_rest(wide_total, experts))
    stream = Stream(gate, wide, wide_sem, SECOND - 3, experts)
    lines = pl.ds(SECOND, 3 * experts - SECOND)
    copies = send_near(1, lines)
    stream.run(SECOND - 3, SECOND - 2, narrow_gate)
    copy = send_across(1, lines, copies)
    mirrored.wait_recv()
    routes = []
    for step in range(1, half):
        for i, route in enumerate((my_route, other_route)):
            at = 1 + 2 * (step - 1) + i
            routes.append(
                post(route, route, route_sent.at[at], route_arrived.at[at], {"rows": half_peer(step)})
            )
    stream.run(SECOND - 2, SECOND - 1, narrow_gate)
    copies = send_back(1, lines, copy)
    for copy in routes:
        copy.wait_recv()
    owner_route = serve_router.at[my_experts, :]
    owner_copies = [
        post(
            owner_route,
            owner_route,
            owner_sent.at[step - 1],
            owner_arrived.at[step - 1],
            {"owner": owner_peer(step)},
        )
        for step in range(1, owners)
    ]
    stream.run(SECOND - 1, SECOND, narrow_gate)
    for copy in copies:
        copy.wait_recv()
    stream.run(SECOND, experts, narrow_gate)
    stream = Stream(up, wide, wide_sem, 0, experts)

    stream.run(0, experts, narrow_wide(rest_scale(experts), 1))
    other.run(0, experts - 1, narrow_down)
    other.run(experts - 1, experts, functools.partial(narrow_down, part_at=last_part_of))

    for which in range(3):
        scale_all[which] = scales[me, which * experts : (which + 1) * experts]
    for expert in range(FIRST):
        scale_all[0, expert : expert + 1, :] = first_scale(expert, me)

    for copy in owner_copies:
        copy.wait_recv()
    for copy in sent_copies:
        copy.wait_send()
    incoming = pl.ds(0, (rows - 1) * depth)
    arrived = (
        final_wide.at[pl.ds(0, experts), incoming, :],
        final_wide.at[pl.ds(experts, experts), incoming, :],
        final_down.at[:, :, pl.ds(0, (rows - 1) * across)],
    )
    sent = (wide_send.at[pl.ds(0, experts)], wide_send.at[pl.ds(experts, experts)], tall_send)
    place = {"rows": row_peer(1)}
    for which in range(3):
        remote(sent[which], sent[which], bulk_sent.at[which], bulk_arrived.at[which], place).wait_send()
    for which in range(3):
        remote(arrived[which], arrived[which], bulk_sent.at[which], bulk_arrived.at[which], place).wait_recv()


def deliver_kernel(wide, down, scale_all, router, gate_out, up_out, down_out, *rest):
    scale_outs, router_out, sems = rest[:3], rest[3], rest[4]
    experts = gate_out.shape[0]
    pairs = [(router, router_out)] + [(scale_all.at[i], scale_outs[i]) for i in range(3)]
    size = experts // PIECES
    for i in range(0, experts, size):
        pairs.append((wide.at[pl.ds(i, size)], gate_out.at[pl.ds(i, size)]))
        pairs.append((wide.at[pl.ds(experts + i, size)], up_out.at[pl.ds(i, size)]))
        pairs.append((down.at[pl.ds(i, size)], down_out.at[pl.ds(i, size)]))
    copies = [pltpu.make_async_copy(*pair, sems.at[i]) for i, pair in enumerate(pairs)]
    for copy in copies:
        copy.start()
    for copy in copies:
        copy.wait()


def serve(
    master_gate,
    second_gate,
    master_up,
    second_up,
    master_down,
    second_down,
    router_weight,
    router_gain,
):
    rows = lax.axis_size("rows")
    owners = lax.axis_size("owner")
    half = rows // 2
    per_rank = rows // half
    experts, depth, columns = master_gate.shape
    _, lines, across = master_down.shape
    width = columns // rows
    tall = lines // rows
    mine = router_weight.shape[1]
    f32, bf16, dma = jnp.float32, jnp.bfloat16, pltpu.SemaphoreType.DMA
    chunks = 3 * experts
    hbm = pl.BlockSpec(memory_space=pltpu.HBM)
    vmem = pl.BlockSpec(memory_space=pltpu.VMEM)
    size = 3 * experts * depth * columns
    arrived = pl.pallas_call(
        serve_kernel,
        out_shape=(
            pltpu.VMEM((2 * experts, rows * depth, width), bf16),
            pltpu.VMEM((experts, tall, rows * across), bf16),
            pltpu.VMEM((3, experts, width), f32),
            pltpu.VMEM((owners * mine, rows * depth), bf16),
        ),
        in_specs=[hbm] * 8,
        out_specs=(vmem,) * 4,
        scratch_shapes=[
            pltpu.VMEM((FIRST, depth, columns), f32),
            pltpu.VMEM((FIRST, depth, columns), bf16),
            pltpu.VMEM((SLOTS, depth, columns), f32),
            pltpu.VMEM((SLOTS, depth, columns), bf16),
            pltpu.VMEM((SLOTS, lines, across), f32),
            pltpu.VMEM((SLOTS, lines, across), bf16),
            pltpu.VMEM((2 * experts, rows - 1, depth, width), bf16),
            pltpu.VMEM((experts, rows - 1, tall, across), bf16),
            pltpu.VMEM((rows, FIRST, rows, LANES), f32),
            pltpu.VMEM((FIRST, rows, LANES), f32),
            pltpu.VMEM((rows, chunks, LANES), f32),
            pltpu.VMEM((half, per_rank, chunks, LANES), f32),
            pltpu.VMEM((per_rank, chunks, LANES), f32),
            pltpu.VMEM((per_rank, chunks, LANES), f32),
            pltpu.VMEM((rows, chunks, LANES), f32),
            pltpu.VMEM((mine, depth), f32),
            pltpu.VMEM((1, depth), f32),
            dma((2, FIRST)),
            dma((2, SLOTS)),
            dma((2, SLOTS)),
            dma((2,)),
            dma((3,)),
            dma((3,)),
            dma((FIRST, rows - 1)),
            dma((FIRST, rows - 1)),
            dma((2, half - 1)),
            dma((2, half - 1)),
            dma((2,)),
            dma((2,)),
            dma((2, half - 1)),
            dma((2, half - 1)),
            dma((2 * half - 1,)),
            dma((2 * half - 1,)),
            dma((owners - 1,)),
            dma((owners - 1,)),
        ],
        compiler_params=pltpu.CompilerParams(
            collective_id=0, has_side_effects=True, vmem_limit_bytes=36 * 1024 * 1024
        ),
        cost_estimate=pl.CostEstimate(flops=8 * size, bytes_accessed=12 * size, transcendentals=0),
    )(
        master_gate,
        second_gate,
        master_up,
        second_up,
        master_down,
        second_down,
        router_weight.T,
        jnp.expand_dims(router_gain, 0),
    )
    outs = pl.pallas_call(
        deliver_kernel,
        out_shape=(
            jax.ShapeDtypeStruct((experts, rows * depth, width), bf16),
            jax.ShapeDtypeStruct((experts, rows * depth, width), bf16),
            jax.ShapeDtypeStruct((experts, tall, rows * across), bf16),
            jax.ShapeDtypeStruct((experts, width), f32),
            jax.ShapeDtypeStruct((experts, width), f32),
            jax.ShapeDtypeStruct((experts, tall), f32),
            jax.ShapeDtypeStruct((owners * mine, rows * depth), bf16),
        ),
        in_specs=[vmem] * 4,
        out_specs=(hbm,) * 7,
        scratch_shapes=[dma((4 + 3 * PIECES,))],
        compiler_params=pltpu.CompilerParams(vmem_limit_bytes=2 * 1024 * 1024),
        cost_estimate=pl.CostEstimate(flops=size, bytes_accessed=4 * size, transcendentals=0),
    )(*arrived)
    return (*outs[:6], outs[6].T)


def serve_fits(experts, depth, columns, lines, across, mine, rows):
    return (
        rows == 8
        and columns // rows == LANES
        and lines // rows == LANES
        and across % LANES == 0
        and depth % LANES == 0
        and experts % 16 == 0
        and mine % 16 == 0
        and experts >= SECOND
    )


def body(
    master_gate,
    second_gate,
    master_up,
    second_up,
    master_down,
    second_down,
    router_weight,
    router_gain,
):
    parts = lax.axis_size("rows")
    if serve_fits(*master_gate.shape, *master_down.shape[1:], router_weight.shape[1], parts):
        return serve(
            master_gate,
            second_gate,
            master_up,
            second_up,
            master_down,
            second_down,
            router_weight,
            router_gain,
        )
    merged_gate = master_gate + second_gate.astype(jnp.float32)
    merged_up = master_up + second_up.astype(jnp.float32)
    merged_down = master_down + second_down.astype(jnp.float32)
    total_gate, total_up, total_down = (
        jnp.sum(lax.all_gather(part, "rows"), axis=0)
        for part in (
            jnp.sum(merged_gate * merged_gate, axis=1),
            jnp.sum(merged_up * merged_up, axis=1),
            jnp.sum(merged_down * merged_down, axis=2),
        )
    )
    part_router = (router_weight * router_gain[:, None]).astype(jnp.bfloat16)
    row_router = lax.all_gather(part_router, "rows", axis=0, tiled=True)
    serve_router = lax.all_gather(row_router, "owner", axis=1, tiled=True)
    total_gate, total_up, total_down, serve_router = lax.optimization_barrier(
        (total_gate, total_up, total_down, serve_router)
    )
    scale_gate = jnp.sqrt(total_gate)
    scale_up = jnp.sqrt(total_up)
    scale_down = jnp.sqrt(total_down)
    final_gate = exchange_columns(narrow_columns(master_gate, second_gate, scale_gate, parts))
    final_up = exchange_columns(narrow_columns(master_up, second_up, scale_up, parts))
    narrow_down = (merged_down / jnp.expand_dims(scale_down, 2)).astype(jnp.bfloat16)
    final_down = lax.all_to_all(narrow_down, "rows", split_axis=1, concat_axis=2, tiled=True)
    scale_gate = lax.dynamic_slice_in_dim(
        scale_gate, lax.axis_index("rows") * final_gate.shape[2], final_gate.shape[2], axis=1
    )
    scale_up = lax.dynamic_slice_in_dim(
        scale_up, lax.axis_index("rows") * final_up.shape[2], final_up.shape[2], axis=1
    )
    scale_down = lax.dynamic_slice_in_dim(
        scale_down, lax.axis_index("rows") * final_down.shape[1], final_down.shape[1], axis=1
    )
    return (final_gate, final_up, final_down, scale_gate, scale_up, scale_down, serve_router)


def solution(mesh):
    placed = (
        P("owner", "rows", None),
        P("owner", "rows", None),
        P("owner", "rows", None),
        P("owner", "rows", None),
        P("owner", None, "rows"),
        P("owner", None, "rows"),
        P("rows", "owner"),
        P("rows"),
    )
    return jax.shard_map(
        body,
        mesh=mesh,
        in_specs=placed,
        out_specs=(
            P("owner", None, "rows"),
            P("owner", None, "rows"),
            P("owner", "rows", None),
            P("owner", "rows"),
            P("owner", "rows"),
            P("owner", "rows"),
            P(),
        ),
        check_vma=False,
    )
```
